8 devices in a mesh: dp: 2 (over z, y), tp: 4 (over x, core).
Axes of the slice: x: 2, y: 2, z: 1, core: 2. Of those that a mesh axis runs over, the one named last changes fastest.
Arguments:
- x_tokens: bfloat16 [8, 1024, 1536], P('dp', 'tp'), parts along dimension 0
- e_time: float32 [8, 3, 1536], P('dp'), parts along dimension 0
- m_block: float32 [3, 1536], replicated
- w_q: bfloat16 [1536, 1536], P(None, 'tp')
- b_q: float32 [1536], P('tp')
- w_k: bfloat16 [1536, 1536], P(None, 'tp')
- b_k: float32 [1536], P('tp')
- w_v: bfloat16 [1536, 1536], P(None, 'tp')
- b_v: float32 [1536], P('tp')
- w_o: bfloat16 [1536, 1536], P('tp')
- b_o: float32 [1536], replicated
- g_q: float32 [1536], P('tp')
- g_k: float32 [1536], P('tp')
- positions: int32 [2048, 3], P('dp'), parts along dimension 0
- d_out: bfloat16 [8, 1024, 1536], P('dp', 'tp'), parts along dimension 0
Outputs:
- output 1: bfloat16 [8, 1024, 1536], P('dp', 'tp'), parts along dimension 0
- output 2: bfloat16 [8, 1024, 1536], P('dp', 'tp'), parts along dimension 0
- output 3: float32 [8, 3, 1536], P('dp'), parts along dimension 0
- output 4: float32 [6, 1536], P('dp'), parts along dimension 0
- output 5: bfloat16 [3072, 1536], P('dp', 'tp'), parts along dimension 0
- output 6: bfloat16 [3072, 1536], P('dp', 'tp'), parts along dimension 0
- output 7: bfloat16 [3072, 1536], P('dp', 'tp'), parts along dimension 0
- output 8: bfloat16 [3072, 1536], P(('dp', 'tp')), parts along dimension 0
- output 9: float32 [3072], P(('dp', 'tp')), parts along dimension 0
- output 10: float32 [3072], P(('dp', 'tp')), parts along dimension 0
There are 2 independent parts. The reference program is written for one: setup_inputs(seed, part) draws one part's arguments, and reference() takes and returns one part's arrays. A program takes and returns all parts, laid end to end along the dimension named above; an argument that names none is the same for every part.
All inputs are finite; a program needn't handle non-finite values.
Results may differ from the reference program's by a relative error of at most 0.0187176.
Values are sent between devices in bfloat16 or wider.
A program may use at most 1 GiB of HBM per device.

```python
import jax
import jax.numpy as jnp
from jax import lax

NUM_BATCH = 4
SEQ_LEN = 1024
NUM_HEADS = 12
HEAD_DIM = 128
MODEL_DIM = 1536
NUM_FRAMES = 21
NUM_ROWS = 45
NUM_COLS = 80

EPS_NORM = 1e-6
ROPE_BASE = 10000.0


def draw_positions(pos_key):
    coord_keys = jax.random.split(pos_key, 3)
    frame_ids = jax.random.randint(coord_keys[0], (SEQ_LEN,), 0, NUM_FRAMES)
    row_ids = jax.random.randint(coord_keys[1], (SEQ_LEN,), 0, NUM_ROWS)
    col_ids = jax.random.randint(coord_keys[2], (SEQ_LEN,), 0, NUM_COLS)
    grid_pos = jnp.stack([frame_ids, row_ids, col_ids], axis=1).astype(jnp.int32)
    corner_hi = jnp.array([NUM_FRAMES - 1, NUM_ROWS - 1, NUM_COLS - 1], dtype=jnp.int32)
    return grid_pos.at[0].set(corner_hi).at[1].set(jnp.zeros((3,), jnp.int32))


def setup_inputs(seed: int = 0, part: int = 0) -> dict:
    root_key = jax.random.key(seed)
    shared_keys = jax.random.split(root_key, 12)
    part_keys = jax.random.split(jax.random.fold_in(root_key, part), 4)
    fan_scale = MODEL_DIM ** -0.5
    head_ramp = 2.0 ** (2.0 * jnp.arange(NUM_HEADS, dtype=jnp.float32) / max(NUM_HEADS - 1, 1) - 1.0)
    col_scale = jnp.repeat(head_ramp, HEAD_DIM)
    sq_shape = (MODEL_DIM, MODEL_DIM)
    vec_shape = (MODEL_DIM,)
    tok_shape = (NUM_BATCH, SEQ_LEN, MODEL_DIM)
    return {
        'x_tokens': (0.5 * jax.random.normal(part_keys[0], tok_shape, jnp.float32)).astype(jnp.bfloat16),
        'e_time': 0.5 * jax.random.normal(part_keys[1], (NUM_BATCH, 3, MODEL_DIM), jnp.float32),
        'm_block': 0.5 * jax.random.normal(shared_keys[0], (3, MODEL_DIM), jnp.float32),
        'w_q': (jax.random.normal(shared_keys[1], sq_shape, jnp.float32) * fan_scale * col_scale).astype(jnp.bfloat16),
        'b_q': 0.5 * jax.random.normal(shared_keys[2], vec_shape, jnp.float32),
        'w_k': (jax.random.normal(shared_keys[3], sq_shape, jnp.float32) * fan_scale * col_scale).astype(jnp.bfloat16),
        'b_k': 0.5 * jax.random.normal(shared_keys[4], vec_shape, jnp.float32),
        'w_v': (jax.random.normal(shared_keys[5], sq_shape, jnp.float32) * (1.5 * fan_scale)).astype(jnp.bfloat16),
        'b_v': 0.5 * jax.random.normal(shared_keys[6], vec_shape, jnp.float32),
        'w_o': (jax.random.normal(shared_keys[7], sq_shape, jnp.float32) * fan_scale).astype(jnp.bfloat16),
        'b_o': 0.5 * jax.random.normal(shared_keys[8], vec_shape, jnp.float32),
        'g_q': jax.random.uniform(shared_keys[9], vec_shape, jnp.float32, 0.5, 1.5),
        'g_k': jax.random.uniform(shared_keys[10], vec_shape, jnp.float32, 0.5, 1.5),
        'positions': draw_positions(part_keys[3]),
        'd_out': jax.random.normal(part_keys[2], tok_shape, jnp.float32).astype(jnp.bfloat16),
    }


def rope_angles(positions):
    half_dim = HEAD_DIM // 2
    side_len = HEAD_DIM // 6
    first_len = half_dim - 2 * side_len
    pair_idx = jnp.arange(half_dim)
    section = (pair_idx >= first_len).astype(jnp.int32) + (pair_idx >= first_len + side_len).astype(jnp.int32)
    offset = jnp.where(section == 0, 0, jnp.where(section == 1, first_len, first_len + side_len))
    sec_width = jnp.where(section == 0, first_len, side_len)
    freq_vals = ROPE_BASE ** (-(pair_idx - offset).astype(jnp.float32) / sec_width.astype(jnp.float32))
    select = jnp.where(section[None, :] == jnp.arange(3)[:, None], freq_vals[None, :], 0.0)
    angles = jnp.sum(positions.astype(jnp.float32)[:, :, None] * select[None, :, :], axis=1)
    return jnp.cos(angles), jnp.sin(angles)


def rope_rotate(values, cos_part, sin_part):
    val_pairs = values.reshape(values.shape[:-1] + (values.shape[-1] // 2, 2))
    even_part = val_pairs[..., 0]
    odd_part = val_pairs[..., 1]
    rotated = jnp.stack([even_part * cos_part - odd_part * sin_part, even_part * sin_part + odd_part * cos_part], axis=-1)
    return rotated.reshape(values.shape)


def full_rms(values, gain):
    return values * lax.rsqrt(jnp.mean(values * values, axis=-1, keepdims=True) + EPS_NORM) * gain


def head_attention(operands):
    q_head, k_head, v_head = operands
    scores = jnp.einsum('bqd,bkd->bqk', q_head.astype(jnp.float32), k_head.astype(jnp.float32)) * HEAD_DIM ** -0.5
    attn_probs = jax.nn.softmax(scores, axis=-1).astype(jnp.bfloat16)
    return jnp.einsum('bqk,bkd->bqd', attn_probs.astype(jnp.float32), v_head.astype(jnp.float32)).astype(jnp.bfloat16)


def attention_block(x_tokens, e_time, m_block, w_q, b_q, w_k, b_k, w_v, b_v, w_o, b_o, g_q, g_k, cos_bcast, sin_bcast):
    head_shape = (NUM_BATCH, SEQ_LEN, NUM_HEADS, HEAD_DIM)
    mod_rows = m_block[None] + e_time
    shift_row = mod_rows[:, 0][:, None]
    scale_one = 1.0 + mod_rows[:, 1][:, None]
    gate_row = mod_rows[:, 2][:, None]
    x_float = x_tokens.astype(jnp.float32)
    centered = x_float - jnp.mean(x_float, axis=-1, keepdims=True)
    x_norm = centered * lax.rsqrt(jnp.mean(centered * centered, axis=-1, keepdims=True) + EPS_NORM)
    y_act = (x_norm * scale_one + shift_row).astype(jnp.bfloat16).reshape(NUM_BATCH * SEQ_LEN, MODEL_DIM)
    q_raw = jnp.dot(y_act, w_q, preferred_element_type=jnp.float32) + b_q
    k_raw = jnp.dot(y_act, w_k, preferred_element_type=jnp.float32) + b_k
    v_heads = (jnp.dot(y_act, w_v, preferred_element_type=jnp.float32) + b_v).astype(jnp.bfloat16).reshape(head_shape)
    q_rot = rope_rotate(full_rms(q_raw, g_q).reshape(head_shape), cos_bcast, sin_bcast).astype(jnp.bfloat16)
    k_rot = rope_rotate(full_rms(k_raw, g_k).reshape(head_shape), cos_bcast, sin_bcast).astype(jnp.bfloat16)
    o_heads = lax.map(jax.checkpoint(head_attention), (jnp.moveaxis(q_rot, 2, 0), jnp.moveaxis(k_rot, 2, 0), jnp.moveaxis(v_heads, 2, 0)))
    o_flat = jnp.moveaxis(o_heads, 0, 2).reshape(NUM_BATCH * SEQ_LEN, MODEL_DIM)
    proj_out = (jnp.dot(o_flat, w_o, preferred_element_type=jnp.float32) + b_o).reshape(NUM_BATCH, SEQ_LEN, MODEL_DIM)
    return (x_float + gate_row * proj_out).astype(jnp.bfloat16)


def reference(x_tokens, e_time, m_block, w_q, b_q, w_k, b_k, w_v, b_v, w_o, b_o, g_q, g_k, positions, d_out):
    cos_tab, sin_tab = rope_angles(positions)
    cos_bcast = cos_tab[None, :, None, :]
    sin_bcast = sin_tab[None, :, None, :]

    def block_fn(x_in, e_in, m_in, wq_in, wk_in, wv_in, wo_in, gq_in, gk_in):
        return attention_block(x_in, e_in, m_in, wq_in, b_q, wk_in, b_k, wv_in, b_v, wo_in, b_o, gq_in, gk_in, cos_bcast, sin_bcast)

    x_out, pull_back = jax.vjp(block_fn, x_tokens, e_time, m_block, w_q, w_k, w_v, w_o, g_q, g_k)
    d_x, d_e, d_m, d_wq, d_wk, d_wv, d_wo, d_gq, d_gk = pull_back(d_out)
    return (x_out, d_x, d_e, d_m, d_wq, d_wk, d_wv, d_wo, d_gq, d_gk)
```

```python
import functools
import math

import jax
import jax.numpy as jnp
from jax import lax
from jax.experimental import pallas as pl
from jax.experimental.pallas import tpu as pltpu
from jax.sharding import PartitionSpec as P


HEAD_DIM = 128
EPS_NORM = 1e-6
ROPE_BASE = 10000.0
F32 = jnp.float32
BF16 = jnp.bfloat16
NT = (((1,), (1,)), ((), ()))
NN = (((1,), (0,)), ((), ()))
TN = (((0,), (0,)), ((), ()))
SCALE = HEAD_DIM ** -0.5
LOG2E = math.log2(math.e)


def rope_angles(positions):
    half_dim = HEAD_DIM // 2
    side_len = HEAD_DIM // 6
    first_len = half_dim - 2 * side_len
    pair_idx = jnp.arange(half_dim)
    section = (pair_idx >= first_len).astype(jnp.int32) + (pair_idx >= first_len + side_len).astype(jnp.int32)
    offset = jnp.where(section == 0, 0, jnp.where(section == 1, first_len, first_len + side_len))
    sec_width = jnp.where(section == 0, first_len, side_len)
    freq_vals = ROPE_BASE ** (-(pair_idx - offset).astype(F32) / sec_width.astype(F32))
    select = jnp.where(section[None, :] == jnp.arange(3)[:, None], freq_vals[None, :], 0.0)
    select = jnp.repeat(select, 2, axis=1)
    angles = jnp.sum(positions.astype(F32)[:, :, None] * select[None, :, :], axis=1)
    sign = jnp.where(jnp.arange(HEAD_DIM) % 2 == 0, -1.0, 1.0)
    return jnp.cos(angles), jnp.sin(angles) * sign


def dot(a, b, dims):
    return lax.dot_general(a, b, dims, preferred_element_type=F32)


def pair_swap(val):
    lane = lax.broadcasted_iota(jnp.int32, val.shape, 1)
    return jnp.where(lane % 2 == 0, pltpu.roll(val, val.shape[1] - 1, 1), pltpu.roll(val, 1, 1))


def col_of(row):
    return jnp.broadcast_to(row, (HEAD_DIM, row.shape[1])).T


def row_of(mat):
    return jnp.sum(mat.T, axis=0, keepdims=True)


def fold_heads(mat, heads):
    out = mat[:, :HEAD_DIM]
    for head in range(1, heads):
        out = out + mat[:, head * HEAD_DIM:(head + 1) * HEAD_DIM]
    return out


def two_rows(first, second):
    sub = lax.broadcasted_iota(jnp.int32, (8, first.shape[1]), 0)
    return jnp.where(sub == 0, first, jnp.where(sub == 1, second, 0.0))


def ln_body(x_ref, dy_ref, mod_ref, y_ref, dp_ref):
    x_val = x_ref[0].astype(F32)
    cen = x_val - jnp.mean(x_val, axis=-1, keepdims=True)
    inv = lax.rsqrt(jnp.mean(cen * cen, axis=-1, keepdims=True) + EPS_NORM)
    y_ref[...] = (cen * inv * (1.0 + mod_ref[0, 1:2]) + mod_ref[0, 0:1]).astype(BF16)
    dp_ref[...] = (dy_ref[0].astype(F32) * mod_ref[0, 2:3]).astype(BF16)


def qkv_body(heads, t_ref, y_ref, wq_ref, wk_ref, wv_ref, bq_ref, bk_ref, bv_ref, q_ref, k_ref, v_ref, st_ref):
    y_val = y_ref[...]
    q_val = dot(y_val, wq_ref[...], NN) + bq_ref[...]
    q_ref[...] = q_val
    k_val = dot(y_val, wk_ref[...], NN) + bk_ref[...]
    k_ref[...] = k_val
    v_ref[...] = (dot(y_val, wv_ref[...], NN) + bv_ref[...]).astype(BF16)
    st_ref[...] = two_rows(row_of(fold_heads(q_val * q_val, heads)), row_of(fold_heads(k_val * k_val, heads)))


def datt_body(t_ref, dp_ref, wo_ref, da_ref):
    da_ref[...] = dot(dp_ref[...], wo_ref[...], NT).astype(BF16)


def total_rows(refs, seq_loc):
    parts = []
    for rel in range(4):
        def piece(k):
            src = rel ^ k
            return refs[k][:, src * seq_loc:(src + 1) * seq_loc]
        parts.append((piece(0) + piece(1)) + (piece(2) + piece(3)))
    return jnp.concatenate(parts, axis=1)


def att_body(heads, model_dim, t_ref, q_ref, k_ref, v_ref, da_ref, cos_ref, sin_ref, s0_ref, s1_ref, s2_ref, s3_ref, gq_ref, gk_ref,
             of_ref, o1_ref, o2_ref, o3_ref, dv_ref, dq_ref, dk_ref, bst_ref, dgq_ref, dgk_ref,
             iq_scr, ik_scr, aq_scr, ak_scr, dqr_scr, qr_scr, kr_scr, vt_scr, kt_scr):
    head = pl.program_id(0)
    seq = q_ref.shape[0]
    blk = seq // 4

    @pl.when(head == 0)
    def _():
        inv = lax.rsqrt(total_rows((s0_ref, s1_ref, s2_ref, s3_ref), blk) / model_dim + EPS_NORM)
        iq_scr[...] = col_of(inv[0:1])
        ik_scr[...] = col_of(inv[1:2])

    cos_val, sin_val = cos_ref[...], sin_ref[...]
    q_hat = q_ref[...] * iq_scr[...]
    q_g = q_hat * gq_ref[...]
    qr_scr[...] = (q_g * cos_val + pair_swap(q_g) * sin_val).astype(BF16)
    k_hat = k_ref[...] * ik_scr[...]
    k_g = k_hat * gk_ref[...]
    k_rot = (k_g * cos_val + pair_swap(k_g) * sin_val).astype(BF16)
    kr_scr[...] = k_rot
    kt_scr[...] = k_rot.T
    vt_scr[...] = v_ref[...].T
    o_refs = (None, o1_ref, o2_ref, o3_ref)
    dv_acc = None
    dk_acc = None
    for i in range(4):
        rows = slice(i * blk, (i + 1) * blk)
        q_i = qr_scr[rows, :]
        do_i = da_ref[rows, :]
        s_t = dot(kr_scr[...], q_i, NT)
        ex = jnp.exp2((s_t - jnp.max(s_t, axis=0, keepdims=True)) * (SCALE * LOG2E))
        prob = ex * (1.0 / jnp.sum(ex, axis=0, keepdims=True))
        pb = prob.astype(BF16)
        o_i = dot(vt_scr[...], pb, NN).T.astype(BF16)
        of_ref[pl.ds(pl.multiple_of((t_ref[0] ^ i) * blk, blk), blk), :] = o_i
        if i:
            o_refs[i][...] = o_i
        dp_t = dot(v_ref[...], do_i, NT)
        delta = jnp.sum(prob * dp_t, axis=0, keepdims=True)
        ds = (prob * (dp_t - delta)).astype(BF16)
        dv_i = dot(pb, do_i, NN)
        dk_i = dot(ds, q_i, NN)
        dv_acc = dv_i if dv_acc is None else dv_acc + dv_i
        dk_acc = dk_i if dk_acc is None else dk_acc + dk_i
        dqr_scr[rows, :] = dot(kt_scr[...], ds, NN).T
    dv_ref[...] = dv_acc.astype(BF16)
    dk_rot = dk_acc * SCALE
    dk_hat = dk_rot * cos_val - pair_swap(dk_rot) * sin_val
    dk_sc = dk_hat * gk_ref[...]
    dk_ref[...] = dk_sc
    dq_rot = dqr_scr[...] * SCALE
    dq_hat = dq_rot * cos_val - pair_swap(dq_rot) * sin_val
    dq_sc = dq_hat * gq_ref[...]
    dq_ref[...] = dq_sc
    dgq_ref[...] = jnp.broadcast_to(jnp.sum(dq_hat * q_hat, axis=0, keepdims=True), (8, HEAD_DIM))
    dgk_ref[...] = jnp.broadcast_to(jnp.sum(dk_hat * k_hat, axis=0, keepdims=True), (8, HEAD_DIM))

    @pl.when(head == 0)
    def _():
        aq_scr[...] = dq_sc * q_hat
        ak_scr[...] = dk_sc * k_hat

    @pl.when(head > 0)
    def _():
        aq_scr[...] += dq_sc * q_hat
        ak_scr[...] += dk_sc * k_hat

    @pl.when(head == heads - 1)
    def _():
        bst_ref[...] = two_rows(row_of(aq_scr[...]), row_of(ak_scr[...]))


def dy_body(heads, model_dim, t_ref, q_ref, k_ref, dq_ref, dk_ref, dv_ref, s0, s1, s2, s3, b0, b1, b2, b3, wq_ref, wk_ref, wv_ref,
            dqr_ref, dkr_ref, dva_ref, c0_ref, c13_ref, c2_ref):
    rel = pl.program_id(0)
    inv = lax.rsqrt(((s0[...] + s1[...]) + (s2[...] + s3[...])) / model_dim + EPS_NORM)
    sgr = ((b0[...] + b1[...]) + (b2[...] + b3[...])) / model_dim

    def wide(row):
        return jnp.concatenate([col_of(row)] * heads, axis=1)

    iq, ik = wide(inv[0:1]), wide(inv[1:2])
    dq_raw = (iq * (dq_ref[...] - q_ref[...] * iq * wide(sgr[0:1]))).astype(BF16)
    dk_raw = (ik * (dk_ref[...] - k_ref[...] * ik * wide(sgr[1:2]))).astype(BF16)
    dv_val = dv_ref[...]
    dqr_ref[...] = dq_raw
    dkr_ref[...] = dk_raw
    dva_ref[...] = dv_val
    out = dot(dq_raw, wq_ref[...], NT) + dot(dk_raw, wk_ref[...], NT) + dot(dv_val, wv_ref[...], NT)

    @pl.when(rel == 0)
    def _():
        c0_ref[...] = out

    @pl.when(rel == 1)
    def _():
        c13_ref[0] = out.astype(BF16)

    @pl.when(rel == 2)
    def _():
        c2_ref[...] = out

    @pl.when(rel == 3)
    def _():
        c13_ref[1] = out.astype(BF16)


def out_body(*refs):
    o_refs = refs[:16]
    w_refs = refs[16:20]
    x_ref, dy_ref, mod_ref, bo_ref, xo_ref, dg_ref = refs[20:]
    for b in range(4):
        @pl.when(pl.program_id(0) == b)
        def _(b=b):
            proj = bo_ref[...]
            for k in range(4):
                proj = proj + dot(o_refs[4 * b + k][...], w_refs[k][...], NN)
            xo_ref[0] = (x_ref[0].astype(F32) + mod_ref[0, 2:3] * proj).astype(BF16)
            dg = jnp.sum(dy_ref[0].astype(F32) * proj, axis=0, keepdims=True)
            dg_ref[0] = jnp.broadcast_to(dg, dg_ref.shape[1:])


def dx_body(c0_ref, rd_ref, rx_ref, x_ref, dy_ref, mod_ref, *rest):
    dx_ref, pm_ref = rest[-2:]
    d_y = (c0_ref[...] + rd_ref[0].astype(F32)) + rx_ref[...].astype(F32)
    x_val = x_ref[0].astype(F32)
    cen = x_val - jnp.mean(x_val, axis=-1, keepdims=True)
    inv = lax.rsqrt(jnp.mean(cen * cen, axis=-1, keepdims=True) + EPS_NORM)
    x_norm = cen * inv
    pm_ref[...] = two_rows(jnp.sum(d_y, axis=0, keepdims=True), jnp.sum(d_y * x_norm, axis=0, keepdims=True))
    d_n = d_y * (1.0 + mod_ref[0, 1:2])
    m1 = jnp.mean(d_n, axis=-1, keepdims=True)
    m2 = jnp.mean(d_n * x_norm, axis=-1, keepdims=True)
    dx_ref[0] = (dy_ref[0].astype(F32) + inv * (d_n - m1 - x_norm * m2)).astype(BF16)


def cost(flops, nbytes):
    return pl.CostEstimate(flops=int(flops), bytes_accessed=int(nbytes), transcendentals=0)


def solution(mesh):
    tp_size = mesh.shape['tp']
    assert tp_size == 4

    def device_step(x_loc, e_loc, m_block, w_q, b_q, w_k, b_k, w_v, b_v, w_o, b_o, g_q, g_k, pos_part, dy_loc):
        nb, sl, dm = x_loc.shape
        seq = sl * tp_size
        hl = w_q.shape[1]
        heads = hl // HEAD_DIM
        t_idx = lax.axis_index('tp')
        t_arr = t_idx.reshape(1).astype(jnp.int32)

        def send(val, k):
            return lax.ppermute(val, 'tp', [(i, i ^ k) for i in range(tp_size)])

        def sds(shape, dtype):
            return jax.ShapeDtypeStruct(shape, dtype)

        def whole(arr):
            nd = arr.ndim
            return pl.BlockSpec(arr.shape, lambda *_: (0,) * nd)

        pos_rel = jnp.concatenate([lax.dynamic_slice_in_dim(pos_part, (t_idx ^ r) * sl, sl, 0) for r in range(4)], axis=0)
        cos_tab, sin_tab = rope_angles(pos_rel)
        mod = m_block[None] + e_loc
        row = lambda a: a.reshape(1, -1)
        bq2, bk2, bv2, bo2, gq2, gk2 = row(b_q), row(b_k), row(b_v), row(b_o), row(g_q), row(g_k)

        ys, dps = [], []
        for b in range(nb):
            y_b, dp_b = pl.pallas_call(
                ln_body, grid=(1,), name="ln",
                in_specs=[pl.BlockSpec((1, sl, dm), lambda i, b=b: (b, 0, 0)), pl.BlockSpec((1, sl, dm), lambda i, b=b: (b, 0, 0)),
                          pl.BlockSpec((1, 3, dm), lambda i, b=b: (b, 0, 0))],
                out_specs=[pl.BlockSpec((sl, dm), lambda i: (0, 0))] * 2,
                out_shape=[sds((sl, dm), BF16)] * 2,
                cost_estimate=cost(2e9, 4 * sl * dm * 2),
            )(x_loc, dy_loc, mod)
            ys.append(y_b)
            dps.append(dp_b)
        y_all, dp_all = [], []
        for b in range(nb):
            y_all.append(lax.all_gather(ys[b], 'tp', axis=0, tiled=True))
            dp_all.append(lax.all_gather(dps[b], 'tp', axis=0, tiled=True))

        wo1 = send(w_o, 1)
        wo2 = send(w_o, 2)
        wo3 = send(wo2, 1)

        rel_in = lambda r, t: (t[0] ^ r, 0)
        rel_blk = lambda r, t: (r, 0)
        fix2 = lambda r, t: (0, 0)

        def qkv(b):
            return pl.pallas_call(
                functools.partial(qkv_body, heads), name="qkv",
                grid_spec=pltpu.PrefetchScalarGridSpec(
                    num_scalar_prefetch=1, grid=(4,),
                    in_specs=[pl.BlockSpec((sl, dm), rel_in)] + [pl.BlockSpec((dm, hl), fix2)] * 3 + [pl.BlockSpec((1, hl), fix2)] * 3,
                    out_specs=[pl.BlockSpec((sl, hl), rel_blk)] * 3 + [pl.BlockSpec((8, sl), lambda r, t: (0, r))]),
                out_shape=[sds((seq, hl), F32), sds((seq, hl), F32), sds((seq, hl), BF16), sds((8, seq), F32)],
                cost_estimate=cost(6 * seq * dm * hl, seq * dm * 2 + 3 * dm * hl * 2 + seq * hl * 10),
            )(t_arr, y_all[b], w_q, w_k, w_v, bq2, bk2, bv2)

        def datt(b):
            return pl.pallas_call(
                datt_body, name="datt",
                grid_spec=pltpu.PrefetchScalarGridSpec(
                    num_scalar_prefetch=1, grid=(4,),
                    in_specs=[pl.BlockSpec((sl, dm), rel_in), pl.BlockSpec((hl, dm), fix2)],
                    out_specs=pl.BlockSpec((sl, hl), rel_blk)),
                out_shape=sds((seq, hl), BF16),
                cost_estimate=cost(2 * seq * dm * hl, seq * dm * 2 + dm * hl * 2 + seq * hl * 2),
            )(t_arr, dp_all[b], w_o)

        def att(q_raw, k_raw, v_val, da, stats):
            hb = pl.BlockSpec((seq, HEAD_DIM), lambda h, t: (0, h))
            ob = pl.BlockSpec((sl, HEAD_DIM), lambda h, t: (0, h))
            gb = pl.BlockSpec((1, HEAD_DIM), lambda h, t: (0, h))
            db = pl.BlockSpec((8, HEAD_DIM), lambda h, t: (0, h))
            tab = pl.BlockSpec((seq, HEAD_DIM), fix2)
            stb = pl.BlockSpec((8, seq), fix2)
            vm = lambda shape, dt: pltpu.VMEM(shape, dt)
            return pl.pallas_call(
                functools.partial(att_body, heads, dm), name="att",
                grid_spec=pltpu.PrefetchScalarGridSpec(
                    num_scalar_prefetch=1, grid=(heads,),
                    in_specs=[hb] * 4 + [tab] * 2 + [stb] * 4 + [gb] * 2,
                    out_specs=[hb, ob, ob, ob, hb, hb, hb, stb, db, db],
                    scratch_shapes=[vm((seq, HEAD_DIM), F32)] * 5 + [vm((seq, HEAD_DIM), BF16)] * 2 + [vm((HEAD_DIM, seq), BF16)] * 2),
                out_shape=[sds((seq, hl), BF16)] + [sds((sl, hl), BF16)] * 3 + [sds((seq, hl), BF16), sds((seq, hl), F32),
                           sds((seq, hl), F32), sds((8, seq), F32), sds((8, hl), F32), sds((8, hl), F32)],
                cost_estimate=cost(24 * seq * seq * hl, seq * hl * 30),
            )(t_arr, q_raw, k_raw, v_val, da, cos_tab, sin_tab, *stats, gq2, gk2)

        def dyk(q_raw, k_raw, dq, dk, dv, stats, bst):
            fb = pl.BlockSpec((sl, hl), rel_blk)
            absb = pl.BlockSpec((sl, hl), rel_in)
            stb = [pl.BlockSpec((8, sl), lambda r, t, k=k: (0, r ^ k)) for k in range(4)]
            return pl.pallas_call(
                functools.partial(dy_body, heads, dm), name="dyk",
                grid_spec=pltpu.PrefetchScalarGridSpec(
                    num_scalar_prefetch=1, grid=(4,),
                    in_specs=[fb] * 5 + stb + stb + [pl.BlockSpec((dm, hl), fix2)] * 3,
                    out_specs=[absb] * 3 + [pl.BlockSpec((sl, dm), fix2), pl.BlockSpec((2, sl, dm), lambda r, t: (0, 0, 0)),
                                            pl.BlockSpec((sl, dm), fix2)]),
                out_shape=[sds((seq, hl), BF16)] * 3 + [sds((sl, dm), F32), sds((2, sl, dm), BF16), sds((sl, dm), F32)],
                cost_estimate=cost(6 * seq * dm * hl, seq * hl * 24 + 3 * dm * hl * 2 + seq * dm * 3),
            )(t_arr, q_raw, k_raw, dq, dk, dv, *stats, *bst, w_q, w_k, w_v)

        def share(val):
            return [val] + [send(val, k) for k in (1, 2, 3)]

        d_gq = 0.0
        d_gk = 0.0
        o_list, dwo, dwq, dwk, dwv, rest = [], 0.0, 0.0, 0.0, 0.0, []
        for b in range(nb):
            q_raw, k_raw, v_val, st = qkv(b)
            stats = share(st)
            da = datt(b)
            of, o1, o2, o3, dv, dq, dk, bs, dgq, dgk = att(q_raw, k_raw, v_val, da, stats)
            d_gq = d_gq + dgq[0]
            d_gk = d_gk + dgk[0]
            bst = share(bs)
            o_list.append((of, send(o1, 1), send(o2, 2), send(o3, 3)))
            dqr, dkr, dva, c0, c13, c2 = dyk(q_raw, k_raw, dq, dk, dv, stats, bst)
            r13 = send(c13, 1)
            rx = send((c2 + r13[1].astype(F32)).astype(BF16), 2)
            rest.append((c0, r13, rx))
            dwo = dwo + dot(of, dp_all[b], TN)
            dwq = dwq + dot(y_all[b], dqr, TN)
            dwk = dwk + dot(y_all[b], dkr, TN)
            dwv = dwv + dot(y_all[b], dva, TN)

        o_in = [o for group in o_list for o in group]
        o_specs = []
        for b in range(nb):
            o_specs.append(pl.BlockSpec((sl, hl), lambda i, t: (t[0], 0)))
            o_specs += [pl.BlockSpec((sl, hl), lambda i, t: (0, 0))] * 3
        tok = pl.BlockSpec((1, sl, dm), lambda i, t: (i, 0, 0))

        def out_wrap(t_ref, *refs):
            out_body(*refs)

        x_out, dgate = pl.pallas_call(
            out_wrap, name="outk",
            grid_spec=pltpu.PrefetchScalarGridSpec(
                num_scalar_prefetch=1, grid=(nb,),
                in_specs=o_specs + [pl.BlockSpec((hl, dm), fix2)] * 4 + [tok, tok, pl.BlockSpec((1, 3, dm), lambda i, t: (i, 0, 0)),
                                                                        pl.BlockSpec((1, dm), fix2)],
                out_specs=[tok, pl.BlockSpec((1, 8, dm), lambda i, t: (i, 0, 0))]),
            out_shape=[sds((nb, sl, dm), BF16), sds((nb, 8, dm), F32)],
            cost_estimate=cost(2 * nb * sl * dm * dm, nb * sl * dm * 8 + dm * dm * 2),
        )(t_arr, *o_in, w_o, wo1, wo2, wo3, x_loc, dy_loc, mod, bo2)

        d_x = None
        pms = []
        for b in range(nb):
            c0, r13, rx = rest[b]
            full = pl.BlockSpec((sl, dm), lambda i: (0, 0))
            tokb = pl.BlockSpec((1, sl, dm), lambda i, b=b: (b, 0, 0))
            ins = [c0, r13, rx, x_loc, dy_loc, mod]
            specs = [full, pl.BlockSpec((1, sl, dm), lambda i: (0, 0, 0)), full, tokb, tokb, pl.BlockSpec((1, 3, dm), lambda i, b=b: (b, 0, 0))]
            alias = {}
            if d_x is not None:
                ins.append(d_x)
                specs.append(pl.BlockSpec(memory_space=pl.ANY))
                alias = {6: 0}
            d_x, pm = pl.pallas_call(
                dx_body, grid=(1,), name="dxk", in_specs=specs,
                out_specs=[tokb, pl.BlockSpec((8, dm), lambda i: (0, 0))],
                out_shape=[sds((nb, sl, dm), BF16), sds((8, dm), F32)],
                input_output_aliases=alias,
                cost_estimate=cost(2e9, sl * dm * 14),
            )(*ins)
            pms.append(pm[:2])
        part = jnp.concatenate([jnp.stack(pms), dgate[:, :1]], axis=1)
        p0, p1, p2, p3 = share(part)
        d_mod = (p0 + p1) + (p2 + p3)
        return (x_out, d_x, d_mod, jnp.sum(d_mod, axis=0), dwq.astype(BF16), dwk.astype(BF16), dwv.astype(BF16), dwo.astype(BF16),
                d_gq, d_gk)

    in_specs = (P('dp', 'tp', None), P('dp', None, None), P(None, None), P(None, 'tp'), P('tp'), P(None, 'tp'), P('tp'),
                P(None, 'tp'), P('tp'), P('tp', None), P(None), P('tp'), P('tp'), P('dp', None), P('dp', 'tp', None))
    out_specs = (P('dp', 'tp', None), P('dp', 'tp', None), P('dp', None, None), P('dp', None), P('dp', 'tp'), P('dp', 'tp'),
                 P('dp', 'tp'), P(('dp', 'tp'), None), P(('dp', 'tp')), P(('dp', 'tp')))
    return jax.shard_map(device_step, mesh=mesh, in_specs=in_specs, out_specs=out_specs, check_vma=False)
```

```python
import functools
import math

import jax
import jax.numpy as jnp
from jax import lax
from jax.experimental import pallas as pl
from jax.experimental.pallas import tpu as pltpu
from jax.sharding import PartitionSpec as P


HEAD_DIM = 128
EPS_NORM = 1e-6
ROPE_BASE = 10000.0
F32 = jnp.float32
BF16 = jnp.bfloat16
NT = (((1,), (1,)), ((), ()))
NN = (((1,), (0,)), ((), ()))
SCALE = HEAD_DIM ** -0.5
LOG2E = math.log2(math.e)


def rope_angles(positions):
    half_dim = HEAD_DIM // 2
    side_len = HEAD_DIM // 6
    first_len = half_dim - 2 * side_len
    pair_idx = jnp.arange(half_dim)
    section = (pair_idx >= first_len).astype(jnp.int32) + (pair_idx >= first_len + side_len).astype(jnp.int32)
    offset = jnp.where(section == 0, 0, jnp.where(section == 1, first_len, first_len + side_len))
    sec_width = jnp.where(section == 0, first_len, side_len)
    freq_vals = ROPE_BASE ** (-(pair_idx - offset).astype(F32) / sec_width.astype(F32))
    select = jnp.where(section[None, :] == jnp.arange(3)[:, None], freq_vals[None, :], 0.0)
    select = jnp.repeat(select, 2, axis=1)
    angles = jnp.sum(positions.astype(F32)[:, :, None] * select[None, :, :], axis=1)
    sign = jnp.where(jnp.arange(HEAD_DIM) % 2 == 0, -1.0, 1.0)
    return jnp.cos(angles), jnp.sin(angles) * sign


def dot(a, b, dims):
    return lax.dot_general(a, b, dims, preferred_element_type=F32)


def pair_swap(val):
    lane = lax.broadcasted_iota(jnp.int32, val.shape, 1)
    return jnp.where(lane % 2 == 0, pltpu.roll(val, val.shape[1] - 1, 1), pltpu.roll(val, 1, 1))


def col_of(row):
    return jnp.broadcast_to(row, (HEAD_DIM, row.shape[1])).T


def row_of(mat):
    return jnp.sum(mat.T, axis=0, keepdims=True)


def fold_heads(mat, heads):
    out = mat[:, :HEAD_DIM]
    for head in range(1, heads):
        out = out + mat[:, head * HEAD_DIM:(head + 1) * HEAD_DIM]
    return out


def two_rows(first, second):
    sub = lax.broadcasted_iota(jnp.int32, (8, first.shape[1]), 0)
    return jnp.where(sub == 0, first, jnp.where(sub == 1, second, 0.0))


def ln_body(x_ref, dy_ref, mod_ref, y_ref, dp_ref):
    x_val = x_ref[0].astype(F32)
    cen = x_val - jnp.mean(x_val, axis=-1, keepdims=True)
    inv = lax.rsqrt(jnp.mean(cen * cen, axis=-1, keepdims=True) + EPS_NORM)
    y_ref[...] = (cen * inv * (1.0 + mod_ref[0, 1:2]) + mod_ref[0, 0:1]).astype(BF16)
    dp_ref[...] = (dy_ref[0].astype(F32) * mod_ref[0, 2:3]).astype(BF16)


def qkv_body(heads, y0, y1, y2, y3, w_ref, bq_ref, bk_ref, bv_ref, q_ref, k_ref, v_ref, st_ref):
    hl = heads * HEAD_DIM
    for rel, y_ref in enumerate((y0, y1, y2, y3)):
        sl = y_ref.shape[0]
        rows = slice(rel * sl, (rel + 1) * sl)
        qkv = dot(y_ref[...], w_ref[...], NN)
        q_val = qkv[:, :hl] + bq_ref[...]
        q_ref[rows, :] = q_val
        k_val = qkv[:, hl:2 * hl] + bk_ref[...]
        k_ref[rows, :] = k_val
        v_ref[rows, :] = (qkv[:, 2 * hl:] + bv_ref[...]).astype(BF16)
        st_ref[:, rows] = two_rows(row_of(fold_heads(q_val * q_val, heads)), row_of(fold_heads(k_val * k_val, heads)))


def total_rows(refs, seq_loc):
    parts = []
    for rel in range(4):
        def piece(k):
            src = rel ^ k
            return refs[k][:, src * seq_loc:(src + 1) * seq_loc]

        parts.append((piece(0) + piece(1)) + (piece(2) + piece(3)))
    return jnp.concatenate(parts, axis=1)


def att_body(heads, model_dim, q_ref, k_ref, v_ref, p0, p1, p2, p3, wot_ref, cos_ref, sin_ref, s0, s1, s2, s3, gq_ref, gk_ref,
             o0_ref, o1_ref, o2_ref, o3_ref, t0_ref, t1_ref, t2_ref, t3_ref, dv_ref, dq_ref, dk_ref, bst_ref, dgq_ref, dgk_ref,
             iq_scr, ik_scr, aq_scr, ak_scr, dqr_scr, qr_scr, kr_scr, vt_scr, kt_scr, da_scr):
    head = pl.program_id(1)
    seq = q_ref.shape[0]
    blk = seq // 4

    @pl.when(head == 0)
    def _():
        inv = lax.rsqrt(total_rows((s0, s1, s2, s3), blk) / model_dim + EPS_NORM)
        iq_scr[...] = col_of(inv[0:1])
        ik_scr[...] = col_of(inv[1:2])
        for rel, p_ref in enumerate((p0, p1, p2, p3)):
            val = dot(p_ref[...], wot_ref[...], NN).astype(BF16)
            for hh in range(heads):
                da_scr[hh, rel * blk:(rel + 1) * blk, :] = val[:, hh * HEAD_DIM:(hh + 1) * HEAD_DIM]

    cos_val, sin_val = cos_ref[...], sin_ref[...]
    q_hat = q_ref[...] * iq_scr[...]
    q_g = q_hat * gq_ref[...]
    qr_scr[...] = (q_g * cos_val + pair_swap(q_g) * sin_val).astype(BF16)
    k_hat = k_ref[...] * ik_scr[...]
    k_g = k_hat * gk_ref[...]
    k_rot = (k_g * cos_val + pair_swap(k_g) * sin_val).astype(BF16)
    kr_scr[...] = k_rot
    kt_scr[...] = k_rot.T
    vt_scr[...] = v_ref[...].T
    o_refs = (o0_ref, o1_ref, o2_ref, o3_ref)
    t_refs = (t0_ref, t1_ref, t2_ref, t3_ref)
    dv_acc = None
    dk_acc = None
    for i in range(4):
        rows = slice(i * blk, (i + 1) * blk)
        q_i = qr_scr[rows, :]
        do_i = da_scr[head, rows, :]
        s_t = dot(kr_scr[...], q_i, NT)
        ex = jnp.exp2((s_t - jnp.max(s_t, axis=0, keepdims=True)) * (SCALE * LOG2E))
        prob = ex * (1.0 / jnp.sum(ex, axis=0, keepdims=True))
        pb = prob.astype(BF16)
        o_t = dot(vt_scr[...], pb, NN).astype(BF16)
        t_refs[i][...] = o_t
        o_refs[i][...] = o_t.T
        dp_t = dot(v_ref[...], do_i, NT)
        delta = jnp.sum(prob * dp_t, axis=0, keepdims=True)
        ds = (prob * (dp_t - delta)).astype(BF16)
        dv_i = dot(pb, do_i, NN)
        dk_i = dot(ds, q_i, NN)
        dv_acc = dv_i if dv_acc is None else dv_acc + dv_i
        dk_acc = dk_i if dk_acc is None else dk_acc + dk_i
        dqr_scr[rows, :] = dot(kt_scr[...], ds, NN).T
    dv_ref[...] = dv_acc.astype(BF16)
    dk_rot = dk_acc * SCALE
    dk_hat = dk_rot * cos_val - pair_swap(dk_rot) * sin_val
    dk_sc = dk_hat * gk_ref[...]
    dk_ref[...] = dk_sc
    dq_rot = dqr_scr[...] * SCALE
    dq_hat = dq_rot * cos_val - pair_swap(dq_rot) * sin_val
    dq_sc = dq_hat * gq_ref[...]
    dq_ref[...] = dq_sc
    dgq_ref[...] = jnp.broadcast_to(jnp.sum(dq_hat * q_hat, axis=0, keepdims=True), (8, HEAD_DIM))
    dgk_ref[...] = jnp.broadcast_to(jnp.sum(dk_hat * k_hat, axis=0, keepdims=True), (8, HEAD_DIM))

    @pl.when(head == 0)
    def _():
        aq_scr[...] = dq_sc * q_hat
        ak_scr[...] = dk_sc * k_hat

    @pl.when(head > 0)
    def _():
        aq_scr[...] += dq_sc * q_hat
        ak_scr[...] += dk_sc * k_hat

    @pl.when(head == heads - 1)
    def _():
        bst_ref[...] = two_rows(row_of(aq_scr[...]), row_of(ak_scr[...]))


def dy_body(heads, model_dim, q_ref, k_ref, dq_ref, dk_ref, dv_ref, s0, s1, s2, s3, b0, b1, b2, b3, wt_ref,
            dt_ref, c0_ref, c1_ref, c2_ref, c3_ref):
    rel = pl.program_id(1)
    inv = lax.rsqrt(((s0[...] + s1[...]) + (s2[...] + s3[...])) / model_dim + EPS_NORM)
    sgr = ((b0[...] + b1[...]) + (b2[...] + b3[...])) / model_dim

    def wide(row):
        return jnp.concatenate([col_of(row)] * heads, axis=1)

    iq, ik = wide(inv[0:1]), wide(inv[1:2])
    dq_raw = (iq * (dq_ref[...] - q_ref[...] * iq * wide(sgr[0:1]))).astype(BF16)
    dk_raw = (ik * (dk_ref[...] - k_ref[...] * ik * wide(sgr[1:2]))).astype(BF16)
    d_cat = jnp.concatenate([dq_raw, dk_raw, dv_ref[...]], axis=1)
    dt_ref[...] = d_cat.T
    out = dot(d_cat, wt_ref[...], NN)
    for k, c_ref in enumerate((c0_ref, c1_ref, c2_ref, c3_ref)):
        @pl.when(rel == k)
        def _(c_ref=c_ref):
            c_ref[...] = out.astype(c_ref.dtype)


def dw_body(groups, n_out, *refs):
    acc = None
    pos = 0
    for n_a, n_z in groups:
        a_val = jnp.concatenate([r[...] for r in refs[pos:pos + n_a]], axis=1) if n_a > 1 else refs[pos][...]
        z_val = jnp.concatenate([r[...] for r in refs[pos + n_a:pos + n_a + n_z]], axis=0)
        pos += n_a + n_z
        part = dot(a_val, z_val, NN)
        acc = part if acc is None else acc + part
    outs = refs[pos:pos + n_out]
    if n_out == 1:
        outs[0][...] = acc.astype(BF16)
    else:
        rows = acc.shape[0] // n_out
        for k in range(n_out):
            outs[k][...] = acc[k * rows:(k + 1) * rows].T.astype(BF16)


def out_body(nbc, n_chunk, *refs):
    n_o = 4 * n_chunk
    o_refs = refs[:n_o]
    w_refs = refs[n_o:n_o + 4]
    x_ref, dy_ref, mod_ref, bo_ref, xo_ref, dg_ref = refs[n_o + 4:]
    for c in range(n_chunk):
        @pl.when(pl.program_id(0) // nbc == c)
        def _(c=c):
            proj = bo_ref[...]
            for k in range(4):
                proj = proj + dot(o_refs[4 * c + k][...], w_refs[k][...], NN)
            xo_ref[0] = (x_ref[0].astype(F32) + mod_ref[0, 2:3] * proj).astype(BF16)
            dg = jnp.sum(dy_ref[0].astype(F32) * proj, axis=0, keepdims=True)
            dg_ref[0] = jnp.broadcast_to(dg, dg_ref.shape[1:])


def dx_body(c0_ref, rd_ref, rx_ref, x_ref, dy_ref, mod_ref, *rest):
    dx_ref, pm_ref = rest[-2:]
    d_y = (c0_ref[...] + rd_ref[...].astype(F32)) + rx_ref[...].astype(F32)
    x_val = x_ref[0].astype(F32)
    cen = x_val - jnp.mean(x_val, axis=-1, keepdims=True)
    inv = lax.rsqrt(jnp.mean(cen * cen, axis=-1, keepdims=True) + EPS_NORM)
    x_norm = cen * inv
    pm_ref[...] = two_rows(jnp.sum(d_y, axis=0, keepdims=True), jnp.sum(d_y * x_norm, axis=0, keepdims=True))
    d_n = d_y * (1.0 + mod_ref[0, 1:2])
    m1 = jnp.mean(d_n, axis=-1, keepdims=True)
    m2 = jnp.mean(d_n * x_norm, axis=-1, keepdims=True)
    dx_ref[0] = (dy_ref[0].astype(F32) + inv * (d_n - m1 - x_norm * m2)).astype(BF16)


def cost(flops, nbytes):
    return pl.CostEstimate(flops=int(flops), bytes_accessed=int(nbytes), transcendentals=0)


def solution(mesh):
    tp_size = mesh.shape['tp']
    assert tp_size == 4
    nbc = 2

    def device_body(x_loc, e_loc, m_block, w_q, b_q, w_k, b_k, w_v, b_v, w_o, b_o, g_q, g_k, pos_part, dy_loc):
        nb, sl, dm = x_loc.shape
        n_chunk = nb // nbc
        seq = sl * tp_size
        hl = w_q.shape[1]
        heads = hl // HEAD_DIM
        rows_p = nbc * sl
        rows_c = nbc * seq
        t_idx = lax.axis_index('tp')

        def send(val, k):
            return lax.ppermute(val, 'tp', [(i, i ^ k) for i in range(tp_size)])

        def sds(shape, dtype):
            return jax.ShapeDtypeStruct(shape, dtype)

        def call(body, grid, ins, in_specs, outs, out_specs, est, scratch=(), alias={}):
            return pl.pallas_call(body, grid=grid, in_specs=in_specs, out_specs=out_specs, out_shape=outs,
                                  scratch_shapes=list(scratch), input_output_aliases=alias, cost_estimate=est)(*ins)

        bs = pl.BlockSpec
        pos_rel = jnp.concatenate([lax.dynamic_slice_in_dim(pos_part, (t_idx ^ r) * sl, sl, 0) for r in range(4)], axis=0)
        cos_tab, sin_tab = rope_angles(pos_rel)
        mod = m_block[None] + e_loc
        row = lambda a: a.reshape(1, -1)
        bq2, bk2, bv2, bo2, gq2, gk2 = row(b_q), row(b_k), row(b_v), row(b_o), row(g_q), row(g_k)
        w_cat = jnp.concatenate([w_q, w_k, w_v], axis=1)
        w_cat_t = w_cat.T
        w_o_t = w_o.T
        fix = lambda *_: (0, 0)

        ys, ps = [], []
        for c in range(n_chunk):
            tokb = bs((1, sl, dm), lambda i, c=c: (c * nbc + i, 0, 0))
            y_c, p_c = call(ln_body, (nbc,), (x_loc, dy_loc, mod),
                            [tokb, tokb, bs((1, 3, dm), lambda i, c=c: (c * nbc + i, 0, 0))],
                            [sds((rows_p, dm), BF16)] * 2, [bs((sl, dm), lambda i: (i, 0))] * 2, cost(4e9, 4 * rows_p * dm * 2))

            def gather(val):
                one = send(val, 1)
                two = send(val, 2)
                return (val, one, two, send(two, 1))

            ys.append(gather(y_c))
            ps.append(gather(p_c))
        wo1 = send(w_o, 1)
        wo2 = send(w_o, 2)
        wo3 = send(wo2, 1)
        pieceb = bs((sl, dm), lambda b, *_: (b, 0))

        def share(val):
            return [val] + [send(val, k) for k in (1, 2, 3)]

        d_gq = 0.0
        d_gk = 0.0
        os_in, ots, dts, rest = [], [], [], []
        for c in range(n_chunk):
            q_raw, k_raw, v_val, st = call(
                functools.partial(qkv_body, heads), (nbc,), (*ys[c], w_cat, bq2, bk2, bv2),
                [pieceb] * 4 + [bs((dm, 3 * hl), fix)] + [bs((1, hl), fix)] * 3,
                [sds((rows_c, hl), F32), sds((rows_c, hl), F32), sds((rows_c, hl), BF16), sds((8, rows_c), F32)],
                [bs((seq, hl), lambda b: (b, 0))] * 3 + [bs((8, seq), lambda b: (0, b))],
                cost(6 * rows_c * dm * hl, rows_c * dm * 2 + 3 * dm * hl * 2 + rows_c * hl * 10))
            stats = share(st)
            hb = bs((seq, HEAD_DIM), lambda b, h: (b, h))
            ob = bs((sl, HEAD_DIM), lambda b, h: (b, h))
            otb = bs((HEAD_DIM, sl), lambda b, h: (h, b))
            gb = bs((1, HEAD_DIM), lambda b, h: (0, h))
            db = bs((8, HEAD_DIM), lambda b, h: (b, h))
            tab = bs((seq, HEAD_DIM), fix)
            stb = bs((8, seq), lambda b, h: (0, b))
            vm = lambda shape, dt: pltpu.VMEM(shape, dt)
            att = call(
                functools.partial(att_body, heads, dm), (nbc, heads),
                (q_raw, k_raw, v_val, *ps[c], w_o_t, cos_tab, sin_tab, *stats, gq2, gk2),
                [hb] * 3 + [pieceb] * 4 + [bs((dm, hl), fix)] + [tab] * 2 + [stb] * 4 + [gb] * 2,
                [sds((rows_p, hl), BF16)] * 4 + [sds((hl, rows_p), BF16)] * 4 + [sds((rows_c, hl), BF16), sds((rows_c, hl), F32),
                 sds((rows_c, hl), F32), sds((8, rows_c), F32), sds((8 * nbc, hl), F32), sds((8 * nbc, hl), F32)],
                [ob] * 4 + [otb] * 4 + [hb, hb, hb, stb, db, db],
                cost(26 * rows_c * seq * hl, rows_c * hl * 30),
                scratch=[vm((seq, HEAD_DIM), F32)] * 5 + [vm((seq, HEAD_DIM), BF16)] * 2 + [vm((HEAD_DIM, seq), BF16)] * 2
                + [vm((heads, seq, HEAD_DIM), BF16)])
            o_own = att[0:4]
            ots.append(att[4:8])
            dv, dq, dk, bst, dgq, dgk = att[8:]
            for b in range(nbc):
                d_gq = d_gq + dgq[8 * b]
                d_gk = d_gk + dgk[8 * b]
            bsts = share(bst)
            os_in += [o_own[0]] + [send(o_own[k], k) for k in (1, 2, 3)]
            fb = bs((sl, hl), lambda b, r: (4 * b + r, 0))
            st_spec = [bs((8, sl), lambda b, r, k=k: (0, 4 * b + (r ^ k))) for k in range(4)]
            cb = bs((sl, dm), lambda b, r: (b, 0))
            d_t, c0, c1, c2, c3 = call(
                functools.partial(dy_body, heads, dm), (nbc, 4),
                (q_raw, k_raw, dq, dk, dv, *stats, *bsts, w_cat_t),
                [fb] * 5 + st_spec + st_spec + [bs((3 * hl, dm), fix)],
                [sds((3 * hl, rows_c), BF16), sds((rows_p, dm), F32), sds((rows_p, dm), BF16), sds((rows_p, dm), F32), sds((rows_p, dm), BF16)],
                [bs((3 * hl, sl), lambda b, r: (0, r * nbc + b))] + [cb] * 4,
                cost(6 * rows_c * dm * hl, rows_c * hl * 24 + 3 * dm * hl * 2 + rows_c * dm * 3))
            dts.append(d_t)
            r3 = send(c3, 1)
            r1 = send(c1, 1)
            rx = send((c2 + r3.astype(F32)).astype(BF16), 2)
            rest.append((c0, r1, rx))

        wide_n = 512
        zb = bs((rows_p, wide_n), lambda j: (0, j))
        args = [a for c in range(n_chunk) for a in (*ots[c], *ps[c])]
        d_wo = call(functools.partial(dw_body, ((4, 4),) * n_chunk, 1), (dm // wide_n,), args,
                    ([bs((hl, rows_p), lambda j: (0, 0))] * 4 + [zb] * 4) * n_chunk, sds((hl, dm), BF16), bs((hl, wide_n), lambda j: (0, j)),
                    cost(2 * n_chunk * rows_c * dm * hl, n_chunk * rows_c * (dm + hl) * 2))
        args = [a for c in range(n_chunk) for a in (dts[c], *ys[c])]
        d_ws = call(functools.partial(dw_body, ((1, 4),) * n_chunk, 3), (dm // wide_n,), args,
                    ([bs((3 * hl, rows_c), lambda j: (0, 0))] + [zb] * 4) * n_chunk, [sds((dm, hl), BF16)] * 3,
                    [bs((wide_n, hl), lambda j: (j, 0))] * 3,
                    cost(6 * n_chunk * rows_c * dm * hl, n_chunk * rows_c * (dm + 3 * hl) * 2))

        o_specs = []
        for c in range(n_chunk):
            o_specs += [bs((sl, hl), lambda i, c=c: (jnp.clip(i - c * nbc, 0, nbc - 1), 0))] * 4
        tok = bs((1, sl, dm), lambda i: (i, 0, 0))
        x_out, dgate = call(
            functools.partial(out_body, nbc, n_chunk), (nb,), (*os_in, w_o, wo1, wo2, wo3, x_loc, dy_loc, mod, bo2),
            o_specs + [bs((hl, dm), fix)] * 4 + [tok, tok, bs((1, 3, dm), lambda i: (i, 0, 0)), bs((1, dm), fix)],
            [sds((nb, sl, dm), BF16), sds((nb, 8, dm), F32)], [tok, bs((1, 8, dm), lambda i: (i, 0, 0))],
            cost(2 * nb * sl * dm * dm, nb * sl * dm * 8 + dm * dm * 2))

        d_x = None
        pms = []
        for c in range(n_chunk):
            c0, r1, rx = rest[c]
            full = bs((sl, dm), lambda i: (i, 0))
            tokb = bs((1, sl, dm), lambda i, c=c: (c * nbc + i, 0, 0))
            ins = [c0, r1, rx, x_loc, dy_loc, mod]
            specs = [full, full, full, tokb, tokb, bs((1, 3, dm), lambda i, c=c: (c * nbc + i, 0, 0))]
            alias = {}
            if d_x is not None:
                ins.append(d_x)
                specs.append(bs(memory_space=pl.ANY))
                alias = {6: 0}
            d_x, pm = call(dx_body, (nbc,), ins, specs, [sds((nb, sl, dm), BF16), sds((8 * nbc, dm), F32)],
                           [tokb, bs((8, dm), lambda i: (i, 0))], cost(4e9, rows_p * dm * 14), alias=alias)
            pms.append(pm.reshape(nbc, 8, dm)[:, :2])
        part = jnp.concatenate([jnp.concatenate(pms, axis=0), dgate[:, :1]], axis=1)
        q0, q1, q2, q3 = share(part)
        d_mod = (q0 + q1) + (q2 + q3)
        return (x_out, d_x, d_mod, jnp.sum(d_mod, axis=0), *d_ws, d_wo, d_gq, d_gk)

    in_specs = (P('dp', 'tp', None), P('dp', None, None), P(None, None), P(None, 'tp'), P('tp'), P(None, 'tp'), P('tp'),
                P(None, 'tp'), P('tp'), P('tp', None), P(None), P('tp'), P('tp'), P('dp', None), P('dp', 'tp', None))
    out_specs = (P('dp', 'tp', None), P('dp', 'tp', None), P('dp', None, None), P('dp', None), P('dp', 'tp'), P('dp', 'tp'),
                 P('dp', 'tp'), P(('dp', 'tp'), None), P(('dp', 'tp')), P(('dp', 'tp')))
    return jax.shard_map(device_body, mesh=mesh, in_specs=in_specs, out_specs=out_specs, check_vma=False)
```

```python
import functools
import math

import jax
import jax.numpy as jnp
from jax import lax
from jax.experimental import pallas as pl
from jax.experimental.pallas import tpu as pltpu
from jax.sharding import PartitionSpec as P


HEAD_DIM = 128
STRIP = 256
EPS_NORM = 1e-6
ROPE_BASE = 10000.0
F32 = jnp.float32
BF16 = jnp.bfloat16
NT = (((1,), (1,)), ((), ()))
NN = (((1,), (0,)), ((), ()))
SCALE = HEAD_DIM ** -0.5
LOG2E = math.log2(math.e)


def rope_angles(positions):
    half_dim = HEAD_DIM // 2
    side_len = HEAD_DIM // 6
    first_len = half_dim - 2 * side_len
    pair_idx = jnp.arange(half_dim)
    section = (pair_idx >= first_len).astype(jnp.int32) + (pair_idx >= first_len + side_len).astype(jnp.int32)
    offset = jnp.where(section == 0, 0, jnp.where(section == 1, first_len, first_len + side_len))
    sec_width = jnp.where(section == 0, first_len, side_len)
    freq_vals = ROPE_BASE ** (-(pair_idx - offset).astype(F32) / sec_width.astype(F32))
    select = jnp.where(section[None, :] == jnp.arange(3)[:, None], freq_vals[None, :], 0.0)
    select = jnp.repeat(select, 2, axis=1)
    angles = jnp.sum(positions.astype(F32)[:, :, None] * select[None, :, :], axis=1)
    sign = jnp.where(jnp.arange(HEAD_DIM) % 2 == 0, -1.0, 1.0)
    return jnp.cos(angles), jnp.sin(angles) * sign


def dot(a, b, dims):
    return lax.dot_general(a, b, dims, preferred_element_type=F32)


def pair_swap(val):
    lane = lax.broadcasted_iota(jnp.int32, val.shape, 1)
    return jnp.where(lane % 2 == 0, pltpu.roll(val, val.shape[1] - 1, 1), pltpu.roll(val, 1, 1))


def col_of(row):
    return jnp.broadcast_to(row, (HEAD_DIM, row.shape[1])).T


def row_of(mat):
    return jnp.sum(mat.T, axis=0, keepdims=True)


def fold_heads(mat, heads):
    out = mat[:, :HEAD_DIM]
    for head in range(1, heads):
        out = out + mat[:, head * HEAD_DIM:(head + 1) * HEAD_DIM]
    return out


def two_rows(first, second):
    sub = lax.broadcasted_iota(jnp.int32, (8, first.shape[1]), 0)
    return jnp.where(sub == 0, first, jnp.where(sub == 1, second, 0.0))


def modulation(e_ref, m_ref):
    return m_ref[...] + e_ref[0]


def ln_value(x_ref, mod):
    x_val = x_ref[0].astype(F32)
    cen = x_val - jnp.mean(x_val, axis=-1, keepdims=True)
    inv = lax.rsqrt(jnp.mean(cen * cen, axis=-1, keepdims=True) + EPS_NORM)
    return (cen * inv * (1.0 + mod[1:2]) + mod[0:1]).astype(BF16)


def lna_body(x_ref, e_ref, m_ref, y_ref):
    y_ref[...] = ln_value(x_ref, modulation(e_ref, m_ref))


def lnb_body(dy_ref, e_ref, m_ref, p_ref):
    mod = modulation(e_ref, m_ref)
    p_ref[...] = (dy_ref[0].astype(F32) * mod[2:3]).astype(BF16)


def lnc_body(x_ref, dy_ref, e_ref, m_ref, y_ref, p_ref):
    mod = modulation(e_ref, m_ref)
    y_ref[...] = ln_value(x_ref, mod)
    p_ref[...] = (dy_ref[0].astype(F32) * mod[2:3]).astype(BF16)


def prep_body(wq_ref, wk_ref, wv_ref, wo_ref, vec_ref, pos_ref, sel_ref, w_ref, wt_ref, wot_ref, vo_ref, cos_ref, sin_ref):
    hl = wq_ref.shape[1]
    for k, ref in enumerate((wq_ref, wk_ref, wv_ref)):
        w_ref[:, k * hl:(k + 1) * hl] = ref[...]
        wt_ref[k * hl:(k + 1) * hl, :] = ref[...].T
    wot_ref[...] = wo_ref[...].T
    vo_ref[...] = vec_ref[...]
    cos_ref[...] = pos_ref[...]
    sin_ref[...] = sel_ref[...]


def qkv_body(heads, first, ya, yb, w_ref, vec_ref, *refs):
    q_ref, k_ref, v_ref, st_ref = refs[-4:]
    hl = heads * HEAD_DIM
    sl = ya.shape[0]
    off = 0
    if not first:
        off = 2 * sl
        st_ref[:, :off] = refs[0][...]
    for rel, y_ref in enumerate((ya, yb)):
        rows = slice(rel * sl, (rel + 1) * sl)
        qkv = dot(y_ref[...], w_ref[...], NN)
        q_val = qkv[:, :hl] + vec_ref[0:1]
        q_ref[rows, :] = q_val
        k_val = qkv[:, hl:2 * hl] + vec_ref[1:2]
        k_ref[rows, :] = k_val
        v_ref[rows, :] = (qkv[:, 2 * hl:] + vec_ref[2:3]).astype(BF16)
        st_ref[:, off + rel * sl:off + (rel + 1) * sl] = two_rows(row_of(fold_heads(q_val * q_val, heads)),
                                                                  row_of(fold_heads(k_val * k_val, heads)))


def datt_body_all(pa0, pb0, pa1, pb1, wot_ref, da_ref):
    sl = pa0.shape[0]
    second = pl.program_id(0) >= pl.num_programs(0) // 2
    for rel, (r0, r1) in enumerate(((pa0, pa1), (pb0, pb1))):
        val = jnp.where(second, r1[...], r0[...])
        da_ref[rel * sl:(rel + 1) * sl, :] = dot(val, wot_ref[...], NN).astype(BF16)


def total_rows(refs, seq_loc):
    parts = []
    for rel in range(4):
        def piece(k):
            src = rel ^ k
            return refs[k][:, src * seq_loc:(src + 1) * seq_loc]

        parts.append((piece(0) + piece(1)) + (piece(2) + piece(3)))
    return jnp.concatenate(parts, axis=1)


def att_body(heads, model_dim, qa_ref, qb_ref, ka_ref, kb_ref, va_ref, vb_ref, da_ref, p2, p3, wot_ref, cos_ref, sin_ref,
             s0, s1, s2, s3, gq_ref, gk_ref,
             o0_ref, o1_ref, o2_ref, o3_ref, t0_ref, t1_ref, t2_ref, t3_ref, dv_ref, dq_ref, dk_ref, bst_ref, dgq_ref, dgk_ref,
             iq_scr, ik_scr, aq_scr, ak_scr, dqr_scr, qh_scr, kh_scr, dva_scr, dka_scr, qr_scr, kr_scr, vv_scr, do_scr, vt_scr, kt_scr,
             da_scr, sa_scr, sb_scr, pa_scr, pb_scr, ea_scr, eb_scr):
    head = pl.program_id(1)
    seq = 2 * qa_ref.shape[0]
    half = seq // 2
    blk = seq // 4

    @pl.when(head == 0)
    def _():
        inv = lax.rsqrt(total_rows((s0, s1, s2, s3), blk) / model_dim + EPS_NORM)
        iq_scr[...] = col_of(inv[0:1])
        ik_scr[...] = col_of(inv[1:2])
        for rel, p_ref in enumerate((p2, p3)):
            val = dot(p_ref[...], wot_ref[...], NN).astype(BF16)
            for hh in range(heads):
                da_scr[hh, rel * blk:(rel + 1) * blk, :] = val[:, hh * HEAD_DIM:(hh + 1) * HEAD_DIM]

    for part, (q_ref, k_ref, v_ref) in enumerate(((qa_ref, ka_ref, va_ref), (qb_ref, kb_ref, vb_ref))):
        rows = slice(part * half, (part + 1) * half)
        cos_val, sin_val = cos_ref[rows, :], sin_ref[rows, :]
        q_hat = q_ref[...] * iq_scr[rows, :]
        qh_scr[rows, :] = q_hat
        q_g = q_hat * gq_ref[...]
        qr_scr[rows, :] = (q_g * cos_val + pair_swap(q_g) * sin_val).astype(BF16)
        k_hat = k_ref[...] * ik_scr[rows, :]
        kh_scr[rows, :] = k_hat
        k_g = k_hat * gk_ref[...]
        k_rot = (k_g * cos_val + pair_swap(k_g) * sin_val).astype(BF16)
        kr_scr[rows, :] = k_rot
        kt_scr[:, rows] = k_rot.T
        vv_scr[rows, :] = v_ref[...]
        vt_scr[:, rows] = v_ref[...].T
    do_scr[:half, :] = da_ref[...]
    do_scr[half:, :] = da_scr[head]
    o_refs = (o0_ref, o1_ref, o2_ref, o3_ref)
    t_refs = (t0_ref, t1_ref, t2_ref, t3_ref)
    s_scr = (sa_scr, sb_scr)
    p_scr = (pa_scr, pb_scr)
    e_scr = (ea_scr, eb_scr)
    strips = [slice(j * STRIP, (j + 1) * STRIP) for j in range(seq // STRIP)]

    def fold_rows(val, op):
        out = val[:8]
        for j in range(1, val.shape[0] // 8):
            out = op(out, val[8 * j:8 * j + 8])
        return out

    def scores(i):
        q_i = qr_scr[i * blk:(i + 1) * blk, :]
        top = None
        for st in strips:
            val = dot(kr_scr[st, :], q_i, NT)
            s_scr[i % 2][st, :] = val
            part = fold_rows(val, jnp.maximum)
            top = part if top is None else jnp.maximum(top, part)
        return jnp.max(top, axis=0, keepdims=True)

    def probs(i, top):
        buf = s_scr[i % 2]
        tot = None
        for st in strips:
            ex = jnp.exp2((buf[st, :] - top) * (SCALE * LOG2E))
            buf[st, :] = ex
            part = fold_rows(ex, jnp.add)
            tot = part if tot is None else tot + part
        inv = 1.0 / jnp.sum(tot, axis=0, keepdims=True)
        for st in strips:
            p_scr[i % 2][st, :] = (buf[st, :] * inv).astype(BF16)
        return inv

    def grads(i, inv):
        rows = slice(i * blk, (i + 1) * blk)
        q_i = qr_scr[rows, :]
        do_i = do_scr[rows, :]
        pb = p_scr[i % 2]
        buf = s_scr[i % 2]
        o_t = dot(vt_scr[...], pb[...], NN)
        o_b = o_t.astype(BF16)
        t_refs[i][...] = o_b
        o_refs[i][...] = o_b.T
        delta = jnp.sum(o_t * do_i.astype(F32).T, axis=0, keepdims=True)
        for st in strips:
            dp_t = dot(vv_scr[st, :], do_i, NT)
            e_scr[i % 2][st, :] = ((buf[st, :] * inv) * (dp_t - delta)).astype(BF16)
        for st in strips:
            dv_i = dot(pb[st, :], do_i, NN)
            dva_scr[st, :] = dv_i if i == 0 else dva_scr[st, :] + dv_i
        for st in strips:
            dk_i = dot(e_scr[i % 2][st, :], q_i, NN)
            dka_scr[st, :] = dk_i if i == 0 else dka_scr[st, :] + dk_i
        dqr_scr[rows, :] = dot(kt_scr[...], e_scr[i % 2][...], NN).T

    top = scores(0)
    for i in range(4):
        nxt = scores(i + 1) if i < 3 else None
        grads(i, probs(i, top))
        top = nxt
    dv_ref[...] = dva_scr[...].astype(BF16)
    gsum_q = None
    gsum_k = None
    for part in range(4):
        rows = slice(part * blk, (part + 1) * blk)
        cos_val, sin_val = cos_ref[rows, :], sin_ref[rows, :]
        dk_rot = dka_scr[rows, :] * SCALE
        dk_hat = dk_rot * cos_val - pair_swap(dk_rot) * sin_val
        dk_sc = dk_hat * gk_ref[...]
        dk_ref[rows, :] = dk_sc
        dq_rot = dqr_scr[rows, :] * SCALE
        dq_hat = dq_rot * cos_val - pair_swap(dq_rot) * sin_val
        dq_sc = dq_hat * gq_ref[...]
        dq_ref[rows, :] = dq_sc
        q_hat = qh_scr[rows, :]
        k_hat = kh_scr[rows, :]
        part_q = fold_rows(dq_hat * q_hat, jnp.add)
        part_k = fold_rows(dk_hat * k_hat, jnp.add)
        gsum_q = part_q if gsum_q is None else gsum_q + part_q
        gsum_k = part_k if gsum_k is None else gsum_k + part_k
        add_q = dq_sc * q_hat
        add_k = dk_sc * k_hat
        aq_scr[rows, :] = jnp.where(head == 0, add_q, aq_scr[rows, :] + add_q)
        ak_scr[rows, :] = jnp.where(head == 0, add_k, ak_scr[rows, :] + add_k)
    dgq_ref[...] = jnp.broadcast_to(jnp.sum(gsum_q, axis=0, keepdims=True), (8, HEAD_DIM))
    dgk_ref[...] = jnp.broadcast_to(jnp.sum(gsum_k, axis=0, keepdims=True), (8, HEAD_DIM))

    @pl.when(head == heads - 1)
    def _():
        bst_ref[...] = two_rows(row_of(aq_scr[...]), row_of(ak_scr[...]))


def dy_body(heads, model_dim, qa_ref, qb_ref, ka_ref, kb_ref, dq_ref, dk_ref, dv_ref, s0, s1, s2, s3, b0, b1, b2, b3, wt_ref,
            t0_ref, t1_ref, t2_ref, t3_ref, c0_ref, c1_ref, c2_ref, c3_ref):
    sl = c0_ref.shape[0]
    inv = lax.rsqrt(total_rows((s0, s1, s2, s3), sl) / model_dim + EPS_NORM)
    sgr = total_rows((b0, b1, b2, b3), sl) / model_dim
    c_refs = (c0_ref, c1_ref, c2_ref, c3_ref)
    t_refs = (t0_ref, t1_ref, t2_ref, t3_ref)

    def wide(row):
        return jnp.concatenate([col_of(row)] * heads, axis=1)

    for rel in (3, 1, 2, 0):
        rows = slice(rel * sl, (rel + 1) * sl)
        src = slice((rel % 2) * sl, (rel % 2 + 1) * sl)
        q_val = (qa_ref, qb_ref)[rel // 2][src, :]
        k_val = (ka_ref, kb_ref)[rel // 2][src, :]
        iq, ik = wide(inv[0:1, rows]), wide(inv[1:2, rows])
        dq_raw = (iq * (dq_ref[rows, :] - q_val * iq * wide(sgr[0:1, rows]))).astype(BF16)
        dk_raw = (ik * (dk_ref[rows, :] - k_val * ik * wide(sgr[1:2, rows]))).astype(BF16)
        d_cat = jnp.concatenate([dq_raw, dk_raw, dv_ref[rows, :]], axis=1)
        t_refs[rel][...] = d_cat.T
        for j in range(3):
            cols = slice(j * 512, (j + 1) * 512)
            c_refs[rel][:, cols] = dot(d_cat, wt_ref[:, cols], NN).astype(c_refs[rel].dtype)


def dw_body(groups, n_out, *refs):
    acc = None
    pos = 0
    for n_a, n_z in groups:
        a_val = jnp.concatenate([r[...] for r in refs[pos:pos + n_a]], axis=1) if n_a > 1 else refs[pos][...]
        z_val = jnp.concatenate([r[...] for r in refs[pos + n_a:pos + n_a + n_z]], axis=0)
        pos += n_a + n_z
        part = dot(a_val, z_val, NN)
        acc = part if acc is None else acc + part
    outs = refs[pos:pos + n_out]
    if n_out == 1:
        outs[0][...] = acc.astype(BF16)
    else:
        rows = acc.shape[0] // n_out
        for k in range(n_out):
            outs[k][...] = acc[k * rows:(k + 1) * rows].T.astype(BF16)


def out_body(nbc, n_chunk, *refs):
    n_o = 4 * n_chunk
    o_refs = refs[:n_o]
    w_refs = refs[n_o:n_o + 4]
    x_ref, dy_ref, e_ref, m_ref, bo_ref, xo_ref, dg_ref = refs[n_o + 4:]
    gate = modulation(e_ref, m_ref)[2:3]
    for c in range(n_chunk):
        @pl.when(pl.program_id(0) // nbc == c)
        def _(c=c):
            proj = bo_ref[...]
            for k in range(4):
                proj = proj + dot(o_refs[4 * c + k][...], w_refs[k][...], NN)
            xo_ref[0] = (x_ref[0].astype(F32) + gate * proj).astype(BF16)
            dg = jnp.sum(dy_ref[0].astype(F32) * proj, axis=0, keepdims=True)
            dg_ref[0] = jnp.broadcast_to(dg, dg_ref.shape[1:])


def dx_body(c0_ref, rd_ref, rx_ref, x_ref, dy_ref, e_ref, m_ref, dg_ref, *rest):
    dx_ref, pm_ref = rest[-2:]
    d_y = (c0_ref[...] + rd_ref[...].astype(F32)) + rx_ref[...].astype(F32)
    x_val = x_ref[0].astype(F32)
    cen = x_val - jnp.mean(x_val, axis=-1, keepdims=True)
    inv = lax.rsqrt(jnp.mean(cen * cen, axis=-1, keepdims=True) + EPS_NORM)
    x_norm = cen * inv
    pm_ref[0, 0:1] = jnp.sum(d_y, axis=0, keepdims=True)
    pm_ref[0, 1:2] = jnp.sum(d_y * x_norm, axis=0, keepdims=True)
    pm_ref[0, 2:3] = dg_ref[0, 0:1]
    d_n = d_y * (1.0 + modulation(e_ref, m_ref)[1:2])
    m1 = jnp.mean(d_n, axis=-1, keepdims=True)
    m2 = jnp.mean(d_n * x_norm, axis=-1, keepdims=True)
    dx_ref[0] = (dy_ref[0].astype(F32) + inv * (d_n - m1 - x_norm * m2)).astype(BF16)


def dm_body(n_chunk, *refs):
    de_ref, dm_ref = refs[-2:]
    nbc = refs[0].shape[0]
    tot = None
    for c in range(n_chunk):
        a, b, d, e = (r[...] for r in refs[4 * c:4 * c + 4])
        val = (a + b) + (d + e)
        de_ref[c * nbc:(c + 1) * nbc] = val
        for k in range(nbc):
            tot = val[k] if tot is None else tot + val[k]
    dm_ref[...] = tot


def cost(flops, nbytes):
    return pl.CostEstimate(flops=int(flops), bytes_accessed=int(nbytes), transcendentals=0)


def solution(mesh):
    tp_size = mesh.shape['tp']
    assert tp_size == 4
    nbc = 2

    def device_body(x_loc, e_loc, m_block, w_q, b_q, w_k, b_k, w_v, b_v, w_o, b_o, g_q, g_k, pos_part, dy_loc):
        nb, sl, dm = x_loc.shape
        n_chunk = nb // nbc
        seq = sl * tp_size
        hl = w_q.shape[1]
        heads = hl // HEAD_DIM
        rows_p = nbc * sl
        rows_c = nbc * seq
        t_idx = lax.axis_index('tp')

        def send(val, k):
            return lax.ppermute(val, 'tp', [(i, i ^ k) for i in range(tp_size)])

        def sds(shape, dtype):
            return jax.ShapeDtypeStruct(shape, dtype)

        def call(body, grid, ins, in_specs, outs, out_specs, est, scratch=(), alias={}):
            return pl.pallas_call(body, grid=grid, in_specs=in_specs, out_specs=out_specs, out_shape=outs,
                                  scratch_shapes=list(scratch), input_output_aliases=alias, cost_estimate=est)(*ins)

        bs = pl.BlockSpec
        pos_rel = jnp.concatenate([lax.dynamic_slice_in_dim(pos_part, (t_idx ^ r) * sl, sl, 0) for r in range(4)], axis=0)
        cos_in, sin_in = rope_angles(pos_rel)
        vec_in = jnp.concatenate([jnp.stack([b_q, b_k, b_v, g_q, g_k]), jnp.zeros((3, hl), F32)], axis=0)
        bo2 = b_o.reshape(1, -1)
        fix = lambda *_: (0, 0)
        pieceb = bs((sl, dm), lambda b, *_: (b, 0))
        mspec = bs((3, dm), fix)

        def tokb(c):
            return bs((1, sl, dm), lambda i, *_, c=c: (c * nbc + i, 0, 0))

        def eb(c):
            return bs((1, 3, dm), lambda i, *_, c=c: (c * nbc + i, 0, 0))

        ysd, psd = sds((rows_p, dm), BF16), sds((rows_p, dm), BF16)
        y0 = call(lna_body, (nbc,), (x_loc, e_loc, m_block), [tokb(0), eb(0), mspec], ysd, pieceb, cost(2e9, 4 * rows_p * dm))
        p0 = call(lnb_body, (nbc,), (dy_loc, e_loc, m_block), [tokb(0), eb(0), mspec], psd, pieceb, cost(2e9, 4 * rows_p * dm))
        y1, p1 = call(lnc_body, (nbc,), (x_loc, dy_loc, e_loc, m_block), [tokb(1), tokb(1), eb(1), mspec], [ysd, psd],
                      [pieceb] * 2, cost(4e9, 8 * rows_p * dm))
        whole = lambda a: bs(a.shape, lambda *_: (0, 0))
        prep_in = (w_q, w_k, w_v, w_o, vec_in, cos_in, sin_in)
        prep_out = [sds((dm, 3 * hl), BF16), sds((3 * hl, dm), BF16), sds((dm, hl), BF16), sds((8, hl), F32), sds((seq, HEAD_DIM), F32),
                    sds((seq, HEAD_DIM), F32)]
        w_cat, w_cat_t, w_o_t, vec, cos_tab, sin_tab = call(
            prep_body, (1,), prep_in, [whole(a) for a in prep_in], prep_out, [whole(a) for a in prep_out], cost(6e9, 16e6))

        def gather(val):
            one = send(val, 1)
            two = send(val, 2)
            return (val, one, two, send(two, 1))

        ys = [gather(v) for v in (y0, y1)]
        ps = [gather(v) for v in (p0, p1)]
        wo1 = send(w_o, 1)
        wo2 = send(w_o, 2)
        wo3 = send(wo2, 1)

        def share(val):
            return [val] + [send(val, k) for k in (1, 2, 3)]

        half = seq // 2
        rows_h = nbc * half
        halfb = bs((half, hl), lambda b: (b, 0))
        qshape = [sds((rows_h, hl), F32), sds((rows_h, hl), F32), sds((rows_h, hl), BF16)]

        def qkv(c, first, extra):
            pieces = ys[c][:2] if first else ys[c][2:]
            width = half if first else seq
            return call(functools.partial(qkv_body, heads, first), (nbc,),
                        (*pieces, w_cat, vec, *extra),
                        [pieceb] * 2 + [whole(w_cat), whole(vec)] + [bs((8, half), lambda b: (0, b))] * len(extra),
                        qshape + [sds((8, nbc * width), F32)], [halfb] * 3 + [bs((8, width), lambda b: (0, b))],
                        cost(6 * rows_h * dm * hl, rows_h * dm * 2 + 3 * dm * hl * 2 + rows_h * hl * 10))

        qkv_a = [qkv(c, True, ()) for c in range(n_chunk)]
        das = call(datt_body_all, (n_chunk * nbc,), (*ps[0][:2], *ps[1][:2], w_o_t),
                   [bs((sl, dm), lambda i, c=c: (jnp.clip(i - c * nbc, 0, nbc - 1), 0)) for c in (0, 0, 1, 1)] + [whole(w_o_t)],
                   sds((n_chunk * rows_h, hl), BF16), bs((half, hl), lambda i: (i, 0)),
                   cost(2 * n_chunk * rows_h * dm * hl, n_chunk * rows_h * dm * 2))

        d_gq = 0.0
        d_gk = 0.0
        os_in, ots, dts, rest = [], [], [], []
        for c in range(n_chunk):
            qa, ka, va, st_a = qkv_a[c]
            qb, kb, vb, st = qkv(c, False, (st_a,))
            stats = share(st)
            hb = bs((seq, HEAD_DIM), lambda b, h: (b, h))
            qhb = bs((half, HEAD_DIM), lambda b, h: (b, h))
            dab = bs((half, HEAD_DIM), lambda b, h, c=c: (c * nbc + b, h))
            ob = bs((sl, HEAD_DIM), lambda b, h: (b, h))
            otb = bs((HEAD_DIM, sl), lambda b, h: (h, b))
            db = bs((8, HEAD_DIM), lambda b, h: (b, h))
            stb = bs((8, seq), lambda b, h: (0, b))
            gq_row, gk_row = vec[3:4], vec[4:5]
            gb = bs((1, HEAD_DIM), lambda b, h: (0, h))
            vm = lambda shape, dt: pltpu.VMEM(shape, dt)
            att = call(
                functools.partial(att_body, heads, dm), (nbc, heads),
                (qa, qb, ka, kb, va, vb, das, *ps[c][2:], w_o_t, cos_tab, sin_tab, *stats, gq_row, gk_row),
                [qhb] * 6 + [dab] + [pieceb] * 2 + [whole(w_o_t), whole(cos_tab), whole(sin_tab)] + [stb] * 4 + [gb] * 2,
                [sds((rows_p, hl), BF16)] * 4 + [sds((hl, rows_p), BF16)] * 4 + [sds((rows_c, hl), BF16), sds((rows_c, hl), F32),
                 sds((rows_c, hl), F32), sds((8, rows_c), F32), sds((8 * nbc, hl), F32), sds((8 * nbc, hl), F32)],
                [ob] * 4 + [otb] * 4 + [hb, hb, hb, stb, db, db],
                cost(25 * rows_c * seq * hl, rows_c * hl * 30),
                scratch=[vm((seq, HEAD_DIM), F32)] * 9 + [vm((seq, HEAD_DIM), BF16)] * 4 + [vm((HEAD_DIM, seq), BF16)] * 2
                + [vm((heads, half, HEAD_DIM), BF16)] + [vm((seq, sl), F32)] * 2 + [vm((seq, sl), BF16)] * 4)
            o_own = att[0:4]
            ots.append(att[4:8])
            dv, dq, dk, bst, dgq, dgk = att[8:]
            for b in range(nbc):
                d_gq = d_gq + dgq[8 * b]
                d_gk = d_gk + dgk[8 * b]
            bsts = share(bst)
            os_in += [o_own[0]] + [send(o_own[k], k) for k in (1, 2, 3)]
            fullb = bs((seq, hl), lambda b: (b, 0))
            st1 = bs((8, seq), lambda b: (0, b))
            *d_t, c0, c1, c2, c3 = call(
                functools.partial(dy_body, heads, dm), (nbc,),
                (qa, qb, ka, kb, dq, dk, dv, *stats, *bsts, w_cat_t),
                [halfb] * 4 + [fullb] * 3 + [st1] * 8 + [whole(w_cat_t)],
                [sds((3 * hl, rows_p), BF16)] * 4 + [sds((rows_p, dm), F32), sds((rows_p, dm), BF16), sds((rows_p, dm), F32),
                                                     sds((rows_p, dm), BF16)],
                [bs((3 * hl, sl), lambda b: (0, b))] * 4 + [pieceb] * 4,
                cost(6 * rows_c * dm * hl, rows_c * hl * 24 + 3 * dm * hl * 2 + rows_c * dm * 3))
            dts.append(d_t)
            r3 = send(c3, 1)
            r1 = send(c1, 1)
            rx = send((c2 + r3.astype(F32)).astype(BF16), 2)
            rest.append((c0, r1, rx))

        wide_n = 512
        zb = bs((rows_p, wide_n), lambda j: (0, j))
        args = [a for c in range(n_chunk) for a in (*ots[c], *ps[c])]
        d_wo = call(functools.partial(dw_body, ((4, 4),) * n_chunk, 1), (dm // wide_n,), args,
                    ([bs((hl, rows_p), lambda j: (0, 0))] * 4 + [zb] * 4) * n_chunk, sds((hl, dm), BF16), bs((hl, wide_n), lambda j: (0, j)),
                    cost(2 * n_chunk * rows_c * dm * hl, n_chunk * rows_c * (dm + hl) * 2))
        args = [a for c in range(n_chunk) for a in (*dts[c], *ys[c])]
        d_ws = call(functools.partial(dw_body, ((4, 4),) * n_chunk, 3), (dm // wide_n,), args,
                    ([bs((3 * hl, rows_p), lambda j: (0, 0))] * 4 + [zb] * 4) * n_chunk, [sds((dm, hl), BF16)] * 3,
                    [bs((wide_n, hl), lambda j: (j, 0))] * 3,
                    cost(6 * n_chunk * rows_c * dm * hl, n_chunk * rows_c * (dm + 3 * hl) * 2))

        o_specs = []
        for c in range(n_chunk):
            o_specs += [bs((sl, hl), lambda i, c=c: (jnp.clip(i - c * nbc, 0, nbc - 1), 0))] * 4
        tok = bs((1, sl, dm), lambda i: (i, 0, 0))
        x_out, dgate = call(
            functools.partial(out_body, nbc, n_chunk), (nb,), (*os_in, w_o, wo1, wo2, wo3, x_loc, dy_loc, e_loc, m_block, bo2),
            o_specs + [bs((hl, dm), fix)] * 4 + [tok, tok, bs((1, 3, dm), lambda i: (i, 0, 0)), mspec, bs((1, dm), fix)],
            [sds((nb, sl, dm), BF16), sds((nb, 8, dm), F32)], [tok, bs((1, 8, dm), lambda i: (i, 0, 0))],
            cost(2 * nb * sl * dm * dm, nb * sl * dm * 8 + dm * dm * 2))

        d_x = None
        mods = []
        for c in range(n_chunk):
            c0, r1, rx = rest[c]
            ins = [c0, r1, rx, x_loc, dy_loc, e_loc, m_block, dgate]
            specs = [pieceb, pieceb, pieceb, tokb(c), tokb(c), eb(c), mspec, bs((1, 8, dm), lambda i, c=c: (c * nbc + i, 0, 0))]
            alias = {}
            if d_x is not None:
                ins.append(d_x)
                specs.append(bs(memory_space=pl.ANY))
                alias = {8: 0}
            d_x, pm = call(dx_body, (nbc,), ins, specs, [sds((nb, sl, dm), BF16), sds((nbc, 3, dm), F32)],
                           [tokb(c), bs((1, 3, dm), lambda i: (i, 0, 0))], cost(4e9, rows_p * dm * 14), alias=alias)
            mods += share(pm)
        pm_spec = bs((nbc, 3, dm), lambda i: (0, 0, 0))
        d_mod, d_m = call(functools.partial(dm_body, n_chunk), (1,), mods, [pm_spec] * len(mods),
                          [sds((nb, 3, dm), F32), sds((3, dm), F32)], [bs((nb, 3, dm), lambda i: (0, 0, 0)), mspec], cost(1e6, 1e6))
        return (x_out, d_x, d_mod, d_m, *d_ws, d_wo, d_gq, d_gk)

    in_specs = (P('dp', 'tp', None), P('dp', None, None), P(None, None), P(None, 'tp'), P('tp'), P(None, 'tp'), P('tp'),
                P(None, 'tp'), P('tp'), P('tp', None), P(None), P('tp'), P('tp'), P('dp', None), P('dp', 'tp', None))
    out_specs = (P('dp', 'tp', None), P('dp', 'tp', None), P('dp', None, None), P('dp', None), P('dp', 'tp'), P('dp', 'tp'),
                 P('dp', 'tp'), P(('dp', 'tp'), None), P(('dp', 'tp')), P(('dp', 'tp')))
    return jax.shard_map(device_body, mesh=mesh, in_specs=in_specs, out_specs=out_specs, check_vma=False)
```
